32 devices in a mesh: rep: 4 (over y, x), col: 8 (over z, core).
Axes of the slice: x: 2, y: 2, z: 4, core: 2. Of those that a mesh axis runs over, the one named last changes fastest.
Arguments:
- tables: float32 [2, 256, 32768], P(None, 'col', 'rep'), may hold values from -4 to 4
- accumulator: float32 [2, 32768], P(None, 'rep'), may hold values from 0.1 to 20
- replica_grads: bfloat16 [4, 2, 256, 16384], P('rep', None, 'col'), may hold values from -6 to 6
- block_ids: int32 [2, 128], replicated, may hold values from 0 to 255, as said below
Outputs:
- new_tables: float32 [2, 256, 32768], P(None, 'col', 'rep')
- new_accumulator: float32 [2, 32768], P(None, 'rep')
The draws below stay inside these ranges and needn't reach their ends.
Inputs may be any that keep to these rules, and one draw needn't show every extreme that they name: `block_ids`: the block ids of one table are distinct; each names a block of 128 rows. Splitting the 32768 rows into 4 equal runs, each run holds exactly 32 of a table's touched blocks.
All inputs are finite; a program needn't handle non-finite values.
Results may differ from the reference program's by a relative error of at most 0.0003.
Values sent between devices are 32-bit elements; how exact they have to be, the bound alone decides.
A program may use at most 64 MiB of HBM per device.

```python
import math
import jax
import jax.numpy as jnp
from jax import lax

DIM = 256
TABLES = 2
BLOCK = 128
ROWS_TAB = 32768
SLAB = 16384
REPS = 4
N_REP = 4


def draw_block_ids(key, part):
    per_shard = ROWS_TAB // BLOCK // N_REP
    taken = SLAB // BLOCK // N_REP
    picked = []
    for table in range(TABLES):
        table_key = jax.random.fold_in(key, 17 + table)
        pieces = []
        for shard in range(N_REP):
            order = jax.random.permutation(jax.random.fold_in(table_key, 1000 + shard), per_shard)
            pieces.append(order[:taken].astype(jnp.int32) + shard * per_shard)
        joined = jnp.concatenate(pieces)
        shuffle = jax.random.permutation(jax.random.fold_in(table_key, 5), SLAB // BLOCK)
        picked.append(joined[shuffle])
    return jnp.stack(picked).astype(jnp.int32)


def levels(own_key, dims, shards, least, high):
    def one(dim, shards_of):
        heights = jax.random.uniform(jax.random.fold_in(jax.random.fold_in(own_key, 6), dim), (shards_of,), jnp.float32, least / len(shards), high / len(shards))
        return jnp.repeat(jnp.exp(heights), dims[dim] // shards_of).reshape((-1,) + (1,) * (len(dims) - dim - 1))

    level = one(*shards[0])
    for cut in shards[1:]:
        level = level * one(*cut)
    return level


def centred(stream_key, dims, deviation, limit, cuts=(), dtype=jnp.bfloat16):
    values = jax.random.normal(stream_key, dims, jnp.float32) * deviation
    if len(cuts) > 0:
        values = levels(stream_key, dims, cuts, -0.22, 0.18) * values
    return jnp.clip(values, min=-limit, max=limit).astype(dtype)


def setup_inputs(seed: int = 0) -> dict:
    arg_keys = jax.random.split(jax.random.key(seed), 5)
    tables = centred(arg_keys[0], (TABLES, DIM, ROWS_TAB), 0.5, 4.0, ((1, 8), (2, 4)), jnp.float32)
    accumulator = jnp.clip(jnp.exp(math.log(20.0) - 5.2983174 * jax.random.uniform(arg_keys[1], (TABLES, ROWS_TAB), jnp.float32) ** levels(arg_keys[1], (TABLES, ROWS_TAB), ((1, 4),), -0.2, 0.2)), 0.1, 20.0)
    replica_grads = centred(arg_keys[2], (REPS, TABLES, DIM, SLAB), 1.0, 6.0, ((0, 4), (2, 8)))
    block_ids = draw_block_ids(jax.random.fold_in(arg_keys[4], 71), 0)
    return dict(tables=tables, accumulator=accumulator, replica_grads=replica_grads, block_ids=block_ids)


def reference(tables, accumulator, replica_grads, block_ids):
    grad = lax.optimization_barrier(jnp.sum(replica_grads.astype(jnp.float32), axis=0))
    squares = lax.optimization_barrier(jnp.sum(grad * grad, axis=1)) / DIM
    nblocks = ROWS_TAB // BLOCK
    outs_tab = []
    outs_acc = []
    for table in range(TABLES):
        ids = block_ids[table].astype(jnp.int32)
        blocked = tables[table].reshape(DIM, nblocks, BLOCK)
        old_rows = jnp.take(blocked, ids, axis=1).reshape(DIM, SLAB)
        acc_blocked = accumulator[table].reshape(nblocks, BLOCK)
        old_accum = jnp.take(acc_blocked, ids, axis=0).reshape(SLAB)
        fresh = old_accum + squares[table]
        moved = old_rows - 0.1 * grad[table] / (jnp.sqrt(fresh)[None, :] + 1e-08)
        blocked = blocked.at[:, ids].set(moved.reshape(DIM, SLAB // BLOCK, BLOCK))
        acc_blocked = acc_blocked.at[ids].set(fresh.reshape(SLAB // BLOCK, BLOCK))
        outs_tab.append(blocked.reshape(DIM, ROWS_TAB))
        outs_acc.append(acc_blocked.reshape(ROWS_TAB))
    return (jnp.stack(outs_tab), jnp.stack(outs_acc))
```

```python
import functools
import math

import jax
import jax.numpy as jnp
from jax import lax
from jax.experimental import pallas as pl
from jax.experimental.pallas import tpu as pltpu
from jax.sharding import PartitionSpec as P

BLOCK = 128
MESH = pl.DeviceIdType.MESH
AHEAD = 2


def layout(mesh, shape, n_slab):
    reps, cols = mesh.shape["rep"], mesh.shape["col"]
    inner = math.isqrt(reps)
    while reps % inner:
        inner -= 1
    ntab, width, _ = shape
    per = n_slab // BLOCK // reps
    group = math.gcd(per, 8)
    return dict(reps=reps, cols=cols, inner=inner, outer=reps // inner, ntab=ntab,
                width=width, per=per, group=group, pieces=per // group)


def pack(cfg, order, grads, packed):
    reps, per, group, pieces = cfg["reps"], cfg["per"], cfg["group"], cfg["pieces"]

    def piece(t, g):
        for owner in range(reps):
            for i in range(group):
                at = order[t, owner * per + g * group + i]
                lanes = pl.ds(pl.multiple_of(at * BLOCK, BLOCK), BLOCK)
                packed[t * pieces + g, owner, :, pl.ds(i * BLOCK, BLOCK)] = grads[0, t, :, lanes].astype(jnp.float32)

    for t in range(cfg["ntab"]):
        lax.fori_loop(0, pieces, lambda g, n, t=t: (piece(t, g), n)[1], 0)


def exchange(cfg, packed, total, squares_out, *scratch):
    reps, cols, inner, outer = cfg["reps"], cfg["cols"], cfg["inner"], cfg["outer"]
    ntab, width, per, group = cfg["ntab"], cfg["width"], cfg["per"], cfg["group"]
    pieces = cfg["pieces"]
    (landed, relayed, landed2, sq_all, s1, r1, s2, r2, s3, r3) = scratch
    chunks = ntab * pieces
    me = lax.axis_index("rep")
    my_col = lax.axis_index("col")
    x, y = lax.rem(me, inner), me // inner

    barrier = pltpu.get_barrier_semaphore()
    for f in range(1, inner):
        pl.semaphore_signal(barrier, inc=1, device_id={"rep": y * inner + lax.rem(x + f, inner)}, device_id_type=MESH)
    for f in range(1, outer):
        pl.semaphore_signal(barrier, inc=1, device_id={"rep": lax.rem(y + f, outer) * inner + x}, device_id_type=MESH)
    for f in range(1, cols):
        pl.semaphore_signal(barrier, inc=1, device_id={"col": lax.rem(my_col + f, cols)}, device_id_type=MESH)

    def axes(c):
        return (inner, outer) if c % 2 == 0 else (outer, inner)

    def rank(c, f, s):
        if c % 2 == 0:
            return lax.rem(y + s, outer) * inner + lax.rem(x + f, inner)
        return lax.rem(y + f, outer) * inner + lax.rem(x + s, inner)

    def place(i):
        return pl.ds(pl.multiple_of(i * BLOCK, BLOCK), BLOCK)

    def own(c, owner, i):
        return packed[c, owner, :, place(i)]

    def each(fn):
        lax.fori_loop(0, group, lambda i, n: (fn(i), n)[1], 0, unroll=True)

    def first_copy(c, f, s):
        return pltpu.make_async_remote_copy(
            packed.at[c, rank(c, f, s)], landed.at[c, f - 1, s], s1.at[c, f - 1, s], r1.at[c, f - 1, s],
            device_id={"rep": rank(c, f, 0)}, device_id_type=MESH)

    def second_copy(c, s):
        return pltpu.make_async_remote_copy(
            relayed.at[c, s - 1], landed2.at[c, s - 1], s2.at[c, s - 1], r2.at[c, s - 1],
            device_id={"rep": rank(c, 0, s)}, device_id_type=MESH)

    def square_copy(c, f):
        return pltpu.make_async_remote_copy(
            sq_all.at[c, my_col], sq_all.at[c, my_col], s3.at[c, f - 1], r3.at[c, f - 1],
            device_id={"col": lax.rem(my_col + f, cols)}, device_id_type=MESH)

    def send(c):
        nf, ns = axes(c)
        for s in [*range(1, ns), 0]:
            for f in range(1, nf):
                first_copy(c, f, s).start()

    def relay(c):
        nf, ns = axes(c)
        for s in range(1, ns):
            for f in range(1, nf):
                first_copy(c, f, s).wait_recv()
            owner = rank(c, 0, s)

            def add(i):
                acc = own(c, owner, i)
                for f in range(1, nf):
                    acc = acc + landed[c, f - 1, s, :, place(i)]
                relayed[c, s - 1, :, place(i)] = acc

            each(add)

    def send_relay(c):
        _, ns = axes(c)
        for s in range(1, ns):
            second_copy(c, s).start()

    def finish(c):
        nf, ns = axes(c)
        for f in range(1, nf):
            first_copy(c, f, 0).wait_recv()
        for s in range(1, ns):
            second_copy(c, s).wait_recv()

        def add(i):
            acc = own(c, me, i)
            for f in range(1, nf):
                acc = acc + landed[c, f - 1, 0, :, place(i)]
            for s in range(1, ns):
                acc = acc + landed2[c, s - 1, :, place(i)]
            total[c, :, place(i)] = acc
            sq_all[c, my_col, pl.ds(i, 1), :] = jnp.sum(acc * acc, axis=0, keepdims=True)

        each(add)

    def send_squares(c):
        for f in range(1, cols):
            square_copy(c, f).start()

    def gather_squares(c):
        for f in range(1, cols):
            square_copy(c, f).wait_recv()
        acc = sq_all[c, 0]
        for f in range(1, cols):
            acc = acc + sq_all[c, f]
        squares_out[c] = acc

    pairs = [[c for c in (k, k + 1) if c < chunks] for k in range(0, chunks, 2)]
    steps = len(pairs)

    def at(k, fns):
        if 0 <= k < steps:
            for fn in fns:
                for c in pairs[k]:
                    fn(c)

    greeted = inner - 1 + outer - 1 + cols - 1
    for k in range(steps + AHEAD + 4):
        if k == 0:
            pl.semaphore_wait(barrier, greeted)
        at(k, [send])
        at(k - AHEAD + 1, [relay, send_relay])
        at(k - AHEAD - 0, [finish, send_squares])
        at(k - AHEAD - 1, [gather_squares])

    for c in range(chunks):
        nf, ns = axes(c)
        for s in range(ns):
            for f in range(1, nf):
                first_copy(c, f, s).wait_send()
        for s in range(1, ns):
            second_copy(c, s).wait_send()
        for f in range(1, cols):
            square_copy(c, f).wait_send()


def update(cfg, dim, ids, total, squares, tables, accumulator, new_tables, new_acc,
           tab, acc, step, out_sem):
    ntab, width, per, group = cfg["ntab"], cfg["width"], cfg["per"], cfg["group"]
    pieces = cfg["pieces"]
    local_blocks = tables.shape[2] // BLOCK
    rows = 8
    parts = width // rows
    me = lax.axis_index("rep")

    def window(ref, t, d):
        return ref.at[t, pl.ds(d * rows, rows)]

    def store(t, d):
        return pltpu.make_async_copy(window(tab, t, d), window(new_tables, t, d), out_sem.at[t, d])

    def target(t, i):
        block = ids[t, me * per + i] - me * local_blocks
        return pl.ds(pl.multiple_of(block * BLOCK, BLOCK), BLOCK)

    new_acc[...] = accumulator[...]
    for t in range(ntab):
        for g in range(pieces):
            c = t * pieces + g
            for i in range(group):
                acc[c, pl.ds(i, 1), :] = accumulator[pl.ds(t, 1), target(t, g * group + i)]
            fresh = acc[c] + squares[c] * (1.0 / dim)
            acc[c] = fresh
            step[c] = 0.1 / (jnp.sqrt(fresh) + 1e-8)
            for i in range(group):
                new_acc[pl.ds(t, 1), target(t, g * group + i)] = acc[c, pl.ds(i, 1), :]
    for t in range(ntab):
        for d in range(parts):
            tab[t, pl.ds(d * rows, rows)] = tables[t, pl.ds(d * rows, rows)]
            for g in range(pieces):
                c = t * pieces + g
                for i in range(group):
                    where = target(t, g * group + i)
                    lanes = pl.ds(i * BLOCK, BLOCK)
                    moved = total[c, pl.ds(d * rows, rows), lanes] * step[c, pl.ds(i, 1), :]
                    tab[t, pl.ds(d * rows, rows), where] = tables[t, pl.ds(d * rows, rows), where] - moved
            store(t, d).start()
    for t in range(ntab):
        for d in range(parts):
            store(t, d).wait()


def body(mesh, tables, accumulator, replica_grads, block_ids):
    cfg = layout(mesh, tables.shape, replica_grads.shape[3])
    ntab, width, per, group = cfg["ntab"], cfg["width"], cfg["per"], cfg["group"]
    cols, pieces = cfg["cols"], cfg["pieces"]
    side = max(cfg["inner"], cfg["outer"])
    chunks, span = ntab * pieces, group * BLOCK
    dim = width * cols
    nslab = replica_grads.shape[3]
    nblk = nslab // BLOCK

    place = jnp.sum((block_ids[:, :, None] > block_ids[:, None, :]).astype(jnp.int32), axis=2)
    hit = place[:, None, :] == jnp.arange(nblk, dtype=jnp.int32)[None, :, None]
    order = jnp.sum(jnp.where(hit, jnp.arange(nblk, dtype=jnp.int32)[None, None, :], 0), axis=2)
    ids = jnp.sum(jnp.where(hit, block_ids[:, None, :], 0), axis=2)

    anyspace = pl.BlockSpec(memory_space=pl.ANY)
    vmem = pl.BlockSpec(memory_space=pltpu.VMEM)
    smem = pl.BlockSpec(memory_space=pltpu.SMEM)
    f32 = jnp.float32
    dma = pltpu.SemaphoreType.DMA
    packed = pl.pallas_call(
        functools.partial(pack, cfg),
        out_shape=jax.ShapeDtypeStruct((chunks, cfg["reps"], width, span), f32),
        in_specs=[smem, vmem],
        out_specs=vmem,
        compiler_params=pltpu.CompilerParams(vmem_limit_bytes=12 * 2**20),
        name="pack",
    )(order, replica_grads)
    total, squares = pl.pallas_call(
        functools.partial(exchange, cfg),
        out_shape=(jax.ShapeDtypeStruct((chunks, width, span), f32),
                   jax.ShapeDtypeStruct((chunks, group, BLOCK), f32)),
        in_specs=[vmem],
        out_specs=(vmem, vmem),
        scratch_shapes=[
            pltpu.VMEM((chunks, side - 1, side, width, span), f32),
            pltpu.VMEM((chunks, side - 1, width, span), f32),
            pltpu.VMEM((chunks, side - 1, width, span), f32),
            pltpu.VMEM((chunks, cols, group, BLOCK), f32),
            dma((chunks, side - 1, side)), dma((chunks, side - 1, side)),
            dma((chunks, side - 1)), dma((chunks, side - 1)),
            dma((chunks, cols - 1)), dma((chunks, cols - 1)),
        ],
        compiler_params=pltpu.CompilerParams(
            collective_id=0, has_side_effects=True, vmem_limit_bytes=24 * 2**20),
        name="exchange",
    )(packed)
    rows = 8
    parts = width // rows
    return pl.pallas_call(
        functools.partial(update, cfg, dim),
        out_shape=(jax.ShapeDtypeStruct(tables.shape, f32),
                   jax.ShapeDtypeStruct(accumulator.shape, f32)),
        in_specs=[smem, vmem, vmem, vmem, vmem],
        out_specs=(anyspace, vmem),
        scratch_shapes=[
            pltpu.VMEM(tables.shape, f32),
            pltpu.VMEM((chunks, group, BLOCK), f32),
            pltpu.VMEM((chunks, group, BLOCK), f32),
            dma((ntab, parts)),
        ],
        compiler_params=pltpu.CompilerParams(vmem_limit_bytes=24 * 2**20),
        name="update",
    )(ids, total, squares, tables, accumulator)


def solution(mesh):
    return jax.shard_map(
        functools.partial(body, mesh),
        mesh=mesh,
        in_specs=(P(None, "col", "rep"), P(None, "rep"), P("rep", None, "col", None), P()),
        out_specs=(P(None, "col", "rep"), P(None, "rep")),
        check_vma=False,
    )
```

```python
import functools
import math

import jax
import jax.numpy as jnp
from jax import lax
from jax.experimental import pallas as pl
from jax.experimental.pallas import tpu as pltpu
from jax.sharding import PartitionSpec as P

BLOCK = 128
MESH = pl.DeviceIdType.MESH
GROUP = 16


def layout(mesh, shape, n_slab):
    reps, cols = mesh.shape["rep"], mesh.shape["col"]
    inner = math.isqrt(reps)
    while reps % inner:
        inner -= 1
    ntab, width, _ = shape
    per = n_slab // BLOCK // reps
    group = math.gcd(per, GROUP)
    return dict(reps=reps, cols=cols, inner=inner, outer=reps // inner, ntab=ntab,
                width=width, per=per, group=group, pieces=per // group)


def pack(cfg, block_ids, grads, packed, ids_out, order_vec, order, order_sem):
    reps, per, group, pieces = cfg["reps"], cfg["per"], cfg["group"], cfg["pieces"]
    ntab, nblk = block_ids.shape
    lane = lax.broadcasted_iota(jnp.int32, (nblk, nblk), 1).astype(jnp.float32)
    slot = lax.broadcasted_iota(jnp.int32, (nblk, nblk), 0).astype(jnp.float32)
    for t in range(ntab):
        across = jnp.broadcast_to(block_ids[pl.ds(t, 1), :].astype(jnp.float32), (nblk, nblk))
        down = across.T
        place = jnp.sum(jnp.where(across < down, 1.0, 0.0), axis=1, keepdims=True)
        hit = place == lane
        order_vec[pl.ds(t, 1), :] = jnp.sum(jnp.where(hit, slot, 0.0), axis=0, keepdims=True).astype(jnp.int32)
        ids_out[pl.ds(t, 1), :] = jnp.sum(jnp.where(hit, down, 0.0), axis=0, keepdims=True).astype(jnp.int32)
    to_scalar = pltpu.make_async_copy(order_vec, order, order_sem)
    to_scalar.start()
    to_scalar.wait()

    def piece(t, g):
        for owner in range(reps):
            for i in range(group):
                at = order[t, owner * per + g * group + i]
                lanes = pl.ds(pl.multiple_of(at * BLOCK, BLOCK), BLOCK)
                packed[t * pieces + g, owner, :, pl.ds(i * BLOCK, BLOCK)] = grads[0, t, :, lanes].astype(jnp.float32)

    for t in range(ntab):
        lax.fori_loop(0, pieces, lambda g, n, t=t: (piece(t, g), n)[1], 0)


def exchange(cfg, packed, total, squares_out, *scratch):
    reps, cols, inner, outer = cfg["reps"], cfg["cols"], cfg["inner"], cfg["outer"]
    ntab, width, per, group = cfg["ntab"], cfg["width"], cfg["per"], cfg["group"]
    pieces = cfg["pieces"]
    (landed, relayed, landed2, sq_all, s1, r1, s2, r2, s3, r3) = scratch
    chunks = ntab * pieces
    me = lax.axis_index("rep")
    my_col = lax.axis_index("col")
    x, y = lax.rem(me, inner), me // inner

    barrier = pltpu.get_barrier_semaphore()
    for f in range(1, inner):
        pl.semaphore_signal(barrier, inc=1, device_id={"rep": y * inner + lax.rem(x + f, inner)}, device_id_type=MESH)
    for f in range(1, outer):
        pl.semaphore_signal(barrier, inc=1, device_id={"rep": lax.rem(y + f, outer) * inner + x}, device_id_type=MESH)
    for f in range(1, cols):
        pl.semaphore_signal(barrier, inc=1, device_id={"col": lax.rem(my_col + f, cols)}, device_id_type=MESH)

    def axes(c):
        return (inner, outer) if c % 2 == 0 else (outer, inner)

    def rank(c, f, s):
        if c % 2 == 0:
            return lax.rem(y + s, outer) * inner + lax.rem(x + f, inner)
        return lax.rem(y + f, outer) * inner + lax.rem(x + s, inner)

    def place(i):
        return pl.ds(pl.multiple_of(i * BLOCK, BLOCK), BLOCK)

    def own(c, owner, i):
        return packed[c, owner, :, place(i)]

    def each(fn):
        lax.fori_loop(0, group, lambda i, n: (fn(i), n)[1], 0, unroll=True)

    def first_copy(c, f, s):
        return pltpu.make_async_remote_copy(
            packed.at[c, rank(c, f, s)], landed.at[c, f - 1, s], s1.at[c, f - 1, s], r1.at[c, f - 1, s],
            device_id={"rep": rank(c, f, 0)}, device_id_type=MESH)

    def second_copy(c, s):
        return pltpu.make_async_remote_copy(
            relayed.at[c, s - 1], landed2.at[c, s - 1], s2.at[c, s - 1], r2.at[c, s - 1],
            device_id={"rep": rank(c, 0, s)}, device_id_type=MESH)

    def square_copy(c, f):
        return pltpu.make_async_remote_copy(
            sq_all.at[c, my_col], sq_all.at[c, my_col], s3.at[c, f - 1], r3.at[c, f - 1],
            device_id={"col": lax.rem(my_col + f, cols)}, device_id_type=MESH)

    def send_far(c):
        nf, ns = axes(c)
        for s in range(1, ns):
            for f in range(1, nf):
                first_copy(c, f, s).start()

    def send_near(c):
        for f in range(1, axes(c)[0]):
            first_copy(c, f, 0).start()

    def relay(c):
        nf, ns = axes(c)
        for s in range(1, ns):
            for f in range(1, nf):
                first_copy(c, f, s).wait_recv()
            owner = rank(c, 0, s)

            def add(i):
                acc = own(c, owner, i)
                for f in range(1, nf):
                    acc = acc + landed[c, f - 1, s, :, place(i)]
                relayed[c, s - 1, :, place(i)] = acc

            each(add)

    def send_relay(c):
        _, ns = axes(c)
        for s in range(1, ns):
            second_copy(c, s).start()

    def finish(c):
        nf, ns = axes(c)
        for f in range(1, nf):
            first_copy(c, f, 0).wait_recv()
        for s in range(1, ns):
            second_copy(c, s).wait_recv()

        def add(i):
            acc = own(c, me, i)
            for f in range(1, nf):
                acc = acc + landed[c, f - 1, 0, :, place(i)]
            for s in range(1, ns):
                acc = acc + landed2[c, s - 1, :, place(i)]
            total[c, :, place(i)] = acc
            sq_all[c, my_col, pl.ds(i, 1), :] = jnp.sum(acc * acc, axis=0, keepdims=True)

        each(add)

    def send_squares(c):
        for f in range(1, cols):
            square_copy(c, f).start()

    def gather_squares(c):
        for f in range(1, cols):
            square_copy(c, f).wait_recv()
        acc = sq_all[c, 0]
        for f in range(1, cols):
            acc = acc + sq_all[c, f]
        squares_out[c] = acc

    pairs = [[c for c in (k, k + 1) if c < chunks] for k in range(0, chunks, 2)]
    steps = len(pairs)

    def at(k, fns):
        if 0 <= k < steps:
            for fn in fns:
                for c in pairs[k]:
                    fn(c)

    greeted = inner - 1 + outer - 1 + cols - 1
    pl.semaphore_wait(barrier, greeted)
    for k in range(steps):
        at(k, [send_far])
    for k in range(steps):
        at(k, [send_near])
    for k in range(steps + 2):
        at(k, [relay, send_relay])
        at(k - 1, [finish, send_squares])
        at(k - 2, [gather_squares])

    for c in range(chunks):
        nf, ns = axes(c)
        for s in range(ns):
            for f in range(1, nf):
                first_copy(c, f, s).wait_send()
        for s in range(1, ns):
            second_copy(c, s).wait_send()
        for f in range(1, cols):
            square_copy(c, f).wait_send()


def update(cfg, dim, ids, total, squares, tables, accumulator, new_tables, new_acc,
           tab, acc, step, out_sem):
    ntab, width, per, group = cfg["ntab"], cfg["width"], cfg["per"], cfg["group"]
    pieces = cfg["pieces"]
    local_blocks = tables.shape[2] // BLOCK
    rows = 8
    parts = width // rows
    me = lax.axis_index("rep")

    def window(ref, t, d):
        return ref.at[t, pl.ds(d * rows, rows)]

    def store(t, d):
        return pltpu.make_async_copy(window(tab, t, d), window(new_tables, t, d), out_sem.at[t, d])

    def target(t, i):
        block = ids[t, me * per + i] - me * local_blocks
        return pl.ds(pl.multiple_of(block * BLOCK, BLOCK), BLOCK)

    new_acc[...] = accumulator[...]
    for t in range(ntab):
        for g in range(pieces):
            c = t * pieces + g
            for i in range(group):
                acc[c, pl.ds(i, 1), :] = accumulator[pl.ds(t, 1), target(t, g * group + i)]
            fresh = acc[c] + squares[c] * (1.0 / dim)
            acc[c] = fresh
            step[c] = 0.1 / (jnp.sqrt(fresh) + 1e-8)
            for i in range(group):
                new_acc[pl.ds(t, 1), target(t, g * group + i)] = acc[c, pl.ds(i, 1), :]
    for t in range(ntab):
        for d in range(parts):
            tab[t, pl.ds(d * rows, rows)] = tables[t, pl.ds(d * rows, rows)]
            for g in range(pieces):
                c = t * pieces + g
                for i in range(group):
                    where = target(t, g * group + i)
                    lanes = pl.ds(i * BLOCK, BLOCK)
                    moved = total[c, pl.ds(d * rows, rows), lanes] * step[c, pl.ds(i, 1), :]
                    tab[t, pl.ds(d * rows, rows), where] = tables[t, pl.ds(d * rows, rows), where] - moved
            store(t, d).start()
    for t in range(ntab):
        for d in range(parts):
            store(t, d).wait()


def body(mesh, tables, accumulator, replica_grads, block_ids):
    cfg = layout(mesh, tables.shape, replica_grads.shape[3])
    ntab, width, per, group = cfg["ntab"], cfg["width"], cfg["per"], cfg["group"]
    cols, pieces = cfg["cols"], cfg["pieces"]
    side = max(cfg["inner"], cfg["outer"])
    chunks, span = ntab * pieces, group * BLOCK
    dim = width * cols
    nslab = replica_grads.shape[3]
    nblk = nslab // BLOCK

    anyspace = pl.BlockSpec(memory_space=pl.ANY)
    vmem = pl.BlockSpec(memory_space=pltpu.VMEM)
    smem = pl.BlockSpec(memory_space=pltpu.SMEM)
    f32 = jnp.float32
    dma = pltpu.SemaphoreType.DMA
    packed, ids = pl.pallas_call(
        functools.partial(pack, cfg),
        out_shape=(jax.ShapeDtypeStruct((chunks, cfg["reps"], width, span), f32),
                   jax.ShapeDtypeStruct(block_ids.shape, jnp.int32)),
        in_specs=[vmem, vmem],
        out_specs=(vmem, vmem),
        scratch_shapes=[
            pltpu.VMEM((ntab, nblk), jnp.int32),
            pltpu.SMEM((ntab, nblk), jnp.int32),
            dma(()),
        ],
        compiler_params=pltpu.CompilerParams(vmem_limit_bytes=16 * 2**20),
        name="pack",
    )(block_ids, replica_grads)
    total, squares = pl.pallas_call(
        functools.partial(exchange, cfg),
        out_shape=(jax.ShapeDtypeStruct((chunks, width, span), f32),
                   jax.ShapeDtypeStruct((chunks, group, BLOCK), f32)),
        in_specs=[vmem],
        out_specs=(vmem, vmem),
        scratch_shapes=[
            pltpu.VMEM((chunks, side - 1, side, width, span), f32),
            pltpu.VMEM((chunks, side - 1, width, span), f32),
            pltpu.VMEM((chunks, side - 1, width, span), f32),
            pltpu.VMEM((chunks, cols, group, BLOCK), f32),
            dma((chunks, side - 1, side)), dma((chunks, side - 1, side)),
            dma((chunks, side - 1)), dma((chunks, side - 1)),
            dma((chunks, cols - 1)), dma((chunks, cols - 1)),
        ],
        compiler_params=pltpu.CompilerParams(
            collective_id=0, has_side_effects=True, vmem_limit_bytes=24 * 2**20),
        name="exchange",
    )(packed)
    rows = 8
    parts = width // rows
    return pl.pallas_call(
        functools.partial(update, cfg, dim),
        out_shape=(jax.ShapeDtypeStruct(tables.shape, f32),
                   jax.ShapeDtypeStruct(accumulator.shape, f32)),
        in_specs=[smem, vmem, vmem, vmem, vmem],
        out_specs=(anyspace, vmem),
        scratch_shapes=[
            pltpu.VMEM(tables.shape, f32),
            pltpu.VMEM((chunks, group, BLOCK), f32),
            pltpu.VMEM((chunks, group, BLOCK), f32),
            dma((ntab, parts)),
        ],
        compiler_params=pltpu.CompilerParams(vmem_limit_bytes=24 * 2**20),
        name="update",
    )(ids, total, squares, tables, accumulator)


def solution(mesh):
    return jax.shard_map(
        functools.partial(body, mesh),
        mesh=mesh,
        in_specs=(P(None, "col", "rep"), P(None, "rep"), P("rep", None, "col", None), P()),
        out_specs=(P(None, "col", "rep"), P(None, "rep")),
        check_vma=False,
    )
```
